32 devices in a mesh: tp: 4 (over z), ep: 8 (over y, x, core).
Axes of the slice: x: 2, y: 2, z: 4, core: 2. Of those that a mesh axis runs over, the one named last changes fastest.
Arguments:
- x_in: bfloat16 [24, 1024, 2048], P('ep', 'tp')
- topk_idx: int32 [24, 1024, 6], P('ep', 'tp')
- top_gate: float32 [24, 1024, 6], P('ep', 'tp')
- g_attn: bfloat16 [2048], replicated
- w_q: bfloat16 [2048, 3072], P(None, 'tp')
- w_dkv: bfloat16 [2048, 576], replicated
- g_kv: bfloat16 [512], replicated
- w_ukv: bfloat16 [512, 4096], P(None, 'tp')
- w_o: bfloat16 [2048, 2048], P('tp')
- g_ffn: bfloat16 [2048], replicated
- w_gate: bfloat16 [64, 2048, 1408], P(('tp', 'ep'))
- w_up: bfloat16 [64, 2048, 1408], P(('tp', 'ep'))
- w_down: bfloat16 [64, 1408, 2048], P(('tp', 'ep'))
- ws_gate: bfloat16 [2048, 2816], replicated
- ws_up: bfloat16 [2048, 2816], replicated
- ws_down: bfloat16 [2816, 2048], replicated
Outputs:
- output 1: bfloat16 [24, 1024, 2048], P('ep', 'tp')
- output 2: bfloat16 [24, 1024, 576], P('ep', 'tp')
All inputs are finite; a program needn't handle non-finite values.
Results may differ from the reference program's by a relative error of at most 0.0137867.
Values are sent between devices in bfloat16 or wider.
A program may use at most 1 GiB of HBM per device.

```python
import numpy as np
import jax
import jax.numpy as jnp
from jax import lax

D = 2048
HEADS = 16
KV_RANK = 512
NOPE = 128
ROPE = 64
VDIM = 128
EXPERTS = 64
FF = 1408
SHARED = 2
TOP = 6
BATCH_DEV = 3
SEQ_DEV = 256
TP = 4
EP = 8

BATCH = BATCH_DEV * EP
SEQ = SEQ_DEV * TP
TOK_DEV = BATCH_DEV * SEQ_DEV
MEAN_LOAD = TOK_DEV * TOP // EXPERTS
CAP_DEV = 3 * MEAN_LOAD


def rms_norm(values, gain_vec):
    values32 = values.astype(jnp.float32)
    inv_rms = lax.rsqrt(jnp.mean(values32 * values32, axis=-1, keepdims=True) + 1e-6)
    return (values32 * inv_rms * gain_vec.astype(jnp.float32)).astype(jnp.bfloat16)


def rope_tables(positions, rope_dim):
    half_dim = rope_dim // 2
    inv_freq = 10000.0 ** (-2.0 * jnp.arange(half_dim, dtype=jnp.float32) / rope_dim)
    angles = positions.astype(jnp.float32)[:, None] * inv_freq[None, :]
    return jnp.cos(angles), jnp.sin(angles)


def rotate(values, cos_tab, sin_tab):
    half_dim = values.shape[-1] // 2
    first = values[..., :half_dim].astype(jnp.float32)
    second = values[..., half_dim:].astype(jnp.float32)
    return jnp.concatenate([first * cos_tab - second * sin_tab, second * cos_tab + first * sin_tab], axis=-1).astype(jnp.bfloat16)


def draw_routing(root_key):
    cold_load = MEAN_LOAD // 3
    pattern = np.array([CAP_DEV, cold_load, cold_load, MEAN_LOAD - 2 * cold_load] * (EXPERTS // 4))
    slot_pattern = np.repeat(np.arange(EXPERTS), pattern)
    perm_key, row_key = jax.random.split(root_key)
    expert_perm = jax.random.permutation(perm_key, EXPERTS).astype(jnp.int32)
    grid = expert_perm[slot_pattern].reshape(TOP, TOK_DEV).T
    row_keys = jax.random.split(row_key, TP * EP)
    blocks = jax.vmap(lambda one_key: jax.random.permutation(one_key, grid, axis=0))(row_keys)
    blocks = blocks.reshape(EP, TP, BATCH_DEV, SEQ_DEV, TOP).transpose(0, 2, 1, 3, 4)
    return blocks.reshape(BATCH, SEQ, TOP)


def setup_inputs(seed: int = 0) -> dict:
    root_key = jax.random.key(seed)
    sub_keys = jax.random.split(root_key, 16)

    def draw_normal(which, shape, scale):
        return (jax.random.normal(sub_keys[which], shape, jnp.float32) * scale).astype(jnp.bfloat16)

    def draw_gain(which, gain_len):
        return jax.random.uniform(sub_keys[which], (gain_len,), jnp.float32, 0.5, 1.5).astype(jnp.bfloat16)

    gate_logits = jax.random.normal(sub_keys[2], (BATCH, SEQ, TOP), jnp.float32)
    return {
        'x_in': draw_normal(0, (BATCH, SEQ, D), 1.0),
        'topk_idx': draw_routing(sub_keys[1]),
        'top_gate': jax.nn.softmax(gate_logits, axis=-1),
        'g_attn': draw_gain(3, D),
        'w_q': draw_normal(4, (D, HEADS * (NOPE + ROPE)), 1.5 * D ** -0.5),
        'w_dkv': draw_normal(5, (D, KV_RANK + ROPE), D ** -0.5),
        'g_kv': draw_gain(6, KV_RANK),
        'w_ukv': draw_normal(7, (KV_RANK, HEADS * (NOPE + VDIM)), 1.5 * KV_RANK ** -0.5),
        'w_o': draw_normal(8, (HEADS * VDIM, D), (HEADS * VDIM) ** -0.5),
        'g_ffn': draw_gain(9, D),
        'w_gate': draw_normal(10, (EXPERTS, D, FF), D ** -0.5),
        'w_up': draw_normal(11, (EXPERTS, D, FF), D ** -0.5),
        'w_down': draw_normal(12, (EXPERTS, FF, D), 2.0 * FF ** -0.5),
        'ws_gate': draw_normal(13, (D, SHARED * FF), D ** -0.5),
        'ws_up': draw_normal(14, (D, SHARED * FF), D ** -0.5),
        'ws_down': draw_normal(15, (SHARED * FF, D), (SHARED * FF) ** -0.5),
    }


def reference(x_in, topk_idx, top_gate, g_attn, w_q, w_dkv, g_kv, w_ukv, w_o, g_ffn, w_gate, w_up, w_down, ws_gate, ws_up, ws_down):
    cos_tab, sin_tab = rope_tables(jnp.arange(SEQ), ROPE)
    causal = jnp.arange(SEQ)[:, None] >= jnp.arange(SEQ)[None, :]
    scale = (NOPE + ROPE) ** -0.5

    def attend_request(x_row):
        normed = rms_norm(x_row, g_attn)
        query = jnp.dot(normed, w_q, preferred_element_type=jnp.float32).astype(jnp.bfloat16).reshape(SEQ, HEADS, NOPE + ROPE)
        latent = jnp.dot(normed, w_dkv, preferred_element_type=jnp.float32)
        c_kv = rms_norm(latent[:, :KV_RANK], g_kv)
        k_rope = rotate(latent[:, KV_RANK:], cos_tab, sin_tab)
        key_val = jnp.dot(c_kv, w_ukv, preferred_element_type=jnp.float32).astype(jnp.bfloat16).reshape(SEQ, HEADS, NOPE + VDIM)
        q_rope = rotate(query[:, :, NOPE:], cos_tab[:, None, :], sin_tab[:, None, :])

        def one_head(head_args):
            q_nope_h, q_rope_h, k_nope_h, value_h = head_args
            scores = jnp.dot(q_nope_h, k_nope_h.T, preferred_element_type=jnp.float32) + jnp.dot(q_rope_h, k_rope.T, preferred_element_type=jnp.float32)
            scores = jnp.where(causal, scores * scale, -jnp.inf)
            attn_prob = jax.nn.softmax(scores, axis=-1).astype(jnp.bfloat16)
            return jnp.dot(attn_prob, value_h, preferred_element_type=jnp.float32).astype(jnp.bfloat16)

        heads_out = lax.map(one_head, (query[:, :, :NOPE].transpose(1, 0, 2), q_rope.transpose(1, 0, 2), key_val[:, :, :NOPE].transpose(1, 0, 2), key_val[:, :, NOPE:].transpose(1, 0, 2)))
        merged = heads_out.transpose(1, 0, 2).reshape(SEQ, HEADS * VDIM)
        attn = jnp.dot(merged, w_o, preferred_element_type=jnp.float32).astype(jnp.bfloat16)
        return attn, jnp.concatenate([c_kv, k_rope], axis=-1)

    attn_all, kv_cache = lax.map(attend_request, x_in)
    hidden = (x_in.astype(jnp.float32) + attn_all.astype(jnp.float32)).astype(jnp.bfloat16)
    tok_total = BATCH * SEQ
    normed = rms_norm(hidden, g_ffn).reshape(tok_total, D)
    flat_ids = topk_idx.reshape(tok_total * TOP)
    flat_gate = top_gate.reshape(tok_total * TOP)
    onehot = (flat_ids[:, None] == jnp.arange(EXPERTS)[None, :]).astype(jnp.int32)
    slot_rank = jnp.sum(jnp.cumsum(onehot, axis=0) * onehot, axis=1) - 1
    cap_all = CAP_DEV * TP * EP
    slot_ids = flat_ids * cap_all + slot_rank
    token_of_slot = jnp.full((EXPERTS * cap_all,), tok_total, jnp.int32).at[slot_ids].set(jnp.arange(tok_total * TOP, dtype=jnp.int32) // TOP).reshape(EXPERTS, cap_all)
    gate_of_slot = jnp.zeros((EXPERTS * cap_all,), jnp.float32).at[slot_ids].set(flat_gate).reshape(EXPERTS, cap_all)
    padded = jnp.concatenate([normed, jnp.zeros((1, D), jnp.bfloat16)], axis=0)

    def expert_step(running, expert_args):
        rows, weights, gate_mat, up_mat, down_mat = expert_args
        picked = padded[rows]
        act_gate = jnp.dot(picked, gate_mat, preferred_element_type=jnp.float32)
        act_up = jnp.dot(picked, up_mat, preferred_element_type=jnp.float32)
        act_hidden = (jax.nn.silu(act_gate) * act_up).astype(jnp.bfloat16)
        expert_out = jnp.dot(act_hidden, down_mat, preferred_element_type=jnp.float32).astype(jnp.bfloat16)
        return running.at[rows].add(weights[:, None] * expert_out.astype(jnp.float32)), None

    scan_out = lax.scan(expert_step, jnp.zeros((tok_total + 1, D), jnp.float32), (token_of_slot, gate_of_slot, w_gate, w_up, w_down))
    routed = scan_out[0][:tok_total]
    shared_gate = jnp.dot(normed, ws_gate, preferred_element_type=jnp.float32)
    shared_up = jnp.dot(normed, ws_up, preferred_element_type=jnp.float32)
    shared_act = (jax.nn.silu(shared_gate) * shared_up).astype(jnp.bfloat16)
    shared_out = jnp.dot(shared_act, ws_down, preferred_element_type=jnp.float32)
    y_sum = hidden.reshape(tok_total, D).astype(jnp.float32) + routed + shared_out
    y_out = y_sum.astype(jnp.bfloat16).reshape(BATCH, SEQ, D)
    return y_out, kv_cache
```

```python
import functools

import jax
import jax.numpy as jnp
from jax import lax
from jax.experimental import pallas as pl
from jax.experimental.pallas import tpu as pltpu
from jax.sharding import PartitionSpec as P


F32 = jnp.float32
BF16 = jnp.bfloat16
VMEM_MAX = 67043328
SMALL = 32


def rms_norm(values, gain_vec):
    values32 = values.astype(F32)
    inv_rms = lax.rsqrt(jnp.mean(values32 * values32, axis=-1, keepdims=True) + 1e-6)
    return (values32 * inv_rms * gain_vec.astype(F32)).astype(BF16)


def rope_tables(positions, rope_dim):
    half_dim = rope_dim // 2
    inv_freq = 10000.0 ** (-2.0 * jnp.arange(half_dim, dtype=F32) / rope_dim)
    angles = positions.astype(F32)[:, None] * inv_freq[None, :]
    return jnp.cos(angles), jnp.sin(angles)


def rotate(values, cos_tab, sin_tab):
    half_dim = values.shape[-1] // 2
    first = values[..., :half_dim].astype(F32)
    second = values[..., half_dim:].astype(F32)
    return jnp.concatenate([first * cos_tab - second * sin_tab, second * cos_tab + first * sin_tab], axis=-1).astype(BF16)


def model_dims(w_q, w_dkv, g_kv, w_ukv, w_o):
    kv_rank = g_kv.shape[0]
    rope_dim = w_dkv.shape[1] - kv_rank
    heads = (w_q.shape[1] - w_ukv.shape[1] + w_o.shape[0]) // rope_dim
    return kv_rank, rope_dim, heads, w_q.shape[1] // heads - rope_dim, w_o.shape[0] // heads


def dot32(lhs, rhs):
    return jnp.dot(lhs, rhs, preferred_element_type=F32)


def project_body(first, u_ref, w_ref, o_ref):
    depth, cols = w_ref.shape[1], o_ref.shape[2]
    total = jnp.zeros(o_ref.shape[1:], F32)
    for part in range(u_ref.shape[1] // depth):
        total = total + dot32(u_ref[:, part * depth:(part + 1) * depth], w_ref[0, :, first + part * cols:first + (part + 1) * cols])
    o_ref[0] = total.astype(BF16)


def project(rows, packed, first, cols):
    toks, width = rows.shape
    groups, depth, wide = packed.shape
    return pl.pallas_call(
        functools.partial(project_body, first),
        grid=(groups,),
        in_specs=[pl.BlockSpec((toks, width), lambda g: (0, 0)), pl.BlockSpec((1, depth, wide), lambda g: (g, 0, 0))],
        out_specs=pl.BlockSpec((1, toks, cols), lambda g: (g, 0, 0)),
        out_shape=jax.ShapeDtypeStruct((groups, toks, cols), BF16),
        cost_estimate=pl.CostEstimate(flops=2 * toks * width * groups * cols, bytes_accessed=20_000_000, transcendentals=0),
        name="project",
    )(rows, packed)


def attend_body(nope, rope, vdim, rank, z_ref, q_ref, c0, c1, c2, c3, w_ref, cos_ref, sin_ref, o_ref):
    rows, blk = q_ref.shape[1], c0.shape[1]
    scale = (nope + rope) ** -0.5
    cache = jnp.concatenate([c0[0], c1[0], c2[0], c3[0]], axis=0)
    key_val = dot32(cache[:, :rank], w_ref[0]).astype(BF16)
    k_rope = cache[:, rank:]
    keys = 4 * blk
    key_idx = lax.broadcasted_iota(jnp.int32, (1, keys), 1)
    ahead = key_idx // blk
    plane = z_ref[0] + ahead
    plane = jnp.where(plane >= 4, plane - 4, plane)
    key_pos = plane * blk + key_idx - ahead * blk
    row_pos = z_ref[0] * blk + lax.broadcasted_iota(jnp.int32, (rows, keys), 0)
    causal = row_pos >= key_pos
    cos_tab, sin_tab = cos_ref[...], sin_ref[...]
    contract = (((1,), (1,)), ((), ()))
    for head in range(2):
        base = head * (nope + rope)
        q_nope = q_ref[0, :, base:base + nope]
        q_rope = rotate(q_ref[0, :, base + nope:base + nope + rope], cos_tab, sin_tab)
        start = head * (nope + vdim)
        k_nope, value = key_val[:, start:start + nope], key_val[:, start + nope:start + nope + vdim]
        scores = lax.dot_general(q_nope, k_nope, contract, preferred_element_type=F32)
        scores = scores + lax.dot_general(q_rope, k_rope, contract, preferred_element_type=F32)
        scores = jnp.where(causal, scores * scale, -jnp.inf)
        unnorm = jnp.exp(scores - jnp.max(scores, axis=-1, keepdims=True))
        prob = (unnorm * (1.0 / jnp.sum(unnorm, axis=-1, keepdims=True))).astype(BF16)
        o_ref[:, head * vdim:(head + 1) * vdim] = dot32(prob, value).astype(BF16)


def attend(query, caches, packed, z_one, cos_tab, sin_tab, dims):
    rank, rope, heads, nope, vdim = dims
    bat, blk, wide = caches[0].shape
    _, toks, qcols = query.shape
    rows = toks // bat
    pair = 2 * (nope + rope)
    per = qcols // pair
    kv_cols = 2 * (nope + vdim)
    body = functools.partial(attend_body, nope, rope, vdim, rank)
    return pl.pallas_call(
        body,
        grid=(heads // 2, bat),
        in_specs=[
            pl.BlockSpec(memory_space=pltpu.SMEM),
            pl.BlockSpec((1, rows, pair), lambda h, b: (h // per, b, h % per)),
        ] + [pl.BlockSpec((1, blk, wide), lambda h, b: (b, 0, 0))] * 4 + [
            pl.BlockSpec((1, rank, kv_cols), lambda h, b: (h // per, 0, h % per)),
            pl.BlockSpec((rows, rope // 2), lambda h, b: (0, 0)),
            pl.BlockSpec((rows, rope // 2), lambda h, b: (0, 0)),
        ],
        out_specs=pl.BlockSpec((rows, 2 * vdim), lambda h, b: (b, h)),
        out_shape=jax.ShapeDtypeStruct((toks, heads * vdim), BF16),
        cost_estimate=pl.CostEstimate(flops=60_000_000_000, bytes_accessed=40_000_000, transcendentals=0),
        name="attend",
    )(z_one, query, *caches, packed, cos_tab, sin_tab)


def experts_body(half, small_ref, ids_ref, *refs):
    toks, (gate_a, up_a, down_a, gate_b, up_b, down_b) = refs[:8], refs[8:14]
    outs = refs[14:18]
    tok, gate_up, down, stage, few, tok_sem, in_sem, down_sem, out_sem = refs[18:]
    step = pl.program_id(0)
    width = gate_a.shape[2]
    cap = stage.shape[1]
    tok_count = tok.shape[1]

    def load_gate_up(which):
        slot = which % 2
        src = (gate_a, up_a) if which < 2 else (gate_b, up_b)
        for part in range(2):
            pltpu.make_async_copy(src[part].at[which % 2], gate_up.at[slot, :, part * width:(part + 1) * width], in_sem.at[slot, part]).start()

    def load_down(which):
        src = down_a if which < 2 else down_b
        pltpu.make_async_copy(src.at[which % 2], down.at[which % 2], down_sem.at[which % 2]).start()

    @pl.when(step == 0)
    def _():
        load_gate_up(0)
        for index in range(8):
            pltpu.make_async_copy(toks[index], tok.at[index // 2, (index % 2) * half:(index % 2 + 1) * half], tok_sem.at[index]).start()
        load_down(0)

    for which in range(1, 4):
        @pl.when(step == which - 1)
        def _():
            load_gate_up(which)
            load_down(which)

    @pl.when(step == 0)
    def _():
        for index in range(8):
            pltpu.make_async_copy(toks[index], tok.at[index // 2, (index % 2) * half:(index % 2 + 1) * half], tok_sem.at[index]).wait()

    for which in range(4):
        @pl.when(step == which)
        def _():
            slot = which % 2
            for part in range(2):
                pltpu.make_async_copy(gate_a.at[0], gate_up.at[slot, :, part * width:(part + 1) * width], in_sem.at[slot, part]).wait()
            pltpu.make_async_copy(down_a.at[0], down.at[slot], down_sem.at[slot]).wait()

    now = lax.rem(step, 2)

    def mlp(rows):
        both = dot32(rows, gate_up[now])
        hidden = (jax.nn.silu(both[:, :width]) * both[:, width:]).astype(BF16)
        return dot32(hidden, down[now]).astype(BF16)

    def pick(home, count):
        ids = ids_ref[home, :count, :]
        lane = lax.broadcasted_iota(jnp.int32, ids.shape, 1)
        parts = [jnp.where(ids == lane + 128 * blk, 1.0, 0.0).astype(BF16) for blk in range(tok_count // 128)]
        return dot32(jnp.concatenate(parts, axis=1), tok[home]).astype(BF16)

    is_small = small_ref[step] == 1

    @pl.when(is_small)
    def _():
        few[...] = mlp(jnp.concatenate([pick(home, SMALL) for home in range(4)], axis=0))

    @pl.loop(0, 4)
    def _(home):
        slot = lax.rem(home, 2)

        @pl.when(jnp.logical_or(step > 0, home >= 2))
        def _():
            pltpu.make_async_copy(stage.at[slot], outs[0].at[0], out_sem.at[slot]).wait()

        @pl.when(is_small)
        def _():
            stage[slot, :SMALL, :] = few[pl.ds(pl.multiple_of(home * SMALL, SMALL), SMALL), :]

        @pl.when(jnp.logical_not(is_small))
        def _():
            stage[slot] = mlp(pick(home, cap))

        for which in range(4):
            @pl.when(home == which)
            def _():
                pltpu.make_async_copy(stage.at[slot], outs[which].at[step], out_sem.at[slot]).start()

    @pl.when(step == 3)
    def _():
        for slot in range(2):
            pltpu.make_async_copy(stage.at[slot], outs[0].at[0], out_sem.at[slot]).wait()


def experts(small, ids, toks, weights, cap):
    half, width = toks[0].shape
    ff = weights[0].shape[2]
    hbm = pl.BlockSpec(memory_space=pl.ANY)
    return pl.pallas_call(
        functools.partial(experts_body, half),
        grid=(4,),
        in_specs=[pl.BlockSpec(memory_space=pltpu.SMEM), pl.BlockSpec((4, cap, 128), lambda e: (e, 0, 0))] + [hbm] * 14,
        out_specs=[hbm] * 4,
        out_shape=[jax.ShapeDtypeStruct((4, cap, width), BF16)] * 4,
        scratch_shapes=[
            pltpu.VMEM((4, 2 * half, width), BF16),
            pltpu.VMEM((2, width, 2 * ff), BF16),
            pltpu.VMEM((2, ff, width), BF16),
            pltpu.VMEM((2, cap, width), BF16),
            pltpu.VMEM((4 * SMALL, width), BF16),
            pltpu.SemaphoreType.DMA((8,)),
            pltpu.SemaphoreType.DMA((2, 2)),
            pltpu.SemaphoreType.DMA((2,)),
            pltpu.SemaphoreType.DMA((2,)),
        ],
        compiler_params=pltpu.CompilerParams(vmem_limit_bytes=VMEM_MAX),
        cost_estimate=pl.CostEstimate(flops=60_000_000_000, bytes_accessed=100_000_000, transcendentals=0),
        name="experts",
    )(small, ids, *toks, *weights)


def combine_body(tok_ref, gate_ref, cnt_ref, r0, r1, r2, r3, *rest):
    extra, (out_ref, acc, turn) = rest[:-3], rest[-3:]
    step = pl.program_id(0)
    cap, width = r0.shape[1], r0.shape[2]
    lanes = width // 128
    toks = out_ref.shape[0]

    @pl.when(step == 0)
    def _():
        acc[...] = jnp.zeros_like(acc)

    for which, src in enumerate((r0, r1, r2, r3)):
        @pl.when(step // 4 == which)
        def _():
            @pl.loop(0, (cnt_ref[step] + 15) // 16)
            def _(group):
                first = pl.multiple_of(group * 16, 16)
                rows = src[0, pl.ds(first, 16), :].astype(F32)
                for blk in range(lanes):
                    turn[pl.ds(blk, 16, stride=lanes), :] = rows[:, 128 * blk:128 * (blk + 1)]
                base = step * cap + first
                for part in range(2):
                    spots = [pl.multiple_of(tok_ref[base + 8 * part + r] * lanes, lanes) for r in range(8)]
                    olds = [acc[pl.ds(spot, lanes), :] for spot in spots]
                    news = [olds[r] + gate_ref[base + 8 * part + r] * turn[(8 * part + r) * lanes:(8 * part + r + 1) * lanes, :] for r in range(8)]
                    for r in range(8):
                        acc[pl.ds(spots[r], lanes), :] = news[r]

    @pl.when(step == 15)
    def _():
        @pl.loop(0, toks // 8)
        def _(tile):
            first = pl.multiple_of(tile * 8, 8)
            for blk in range(lanes):
                value = acc[pl.ds(first * lanes + blk, 8, stride=lanes), :]
                for more in extra:
                    value = value + more[pl.ds(first, 8), 128 * blk:128 * (blk + 1)]
                out_ref[pl.ds(first, 8), 128 * blk:128 * (blk + 1)] = value


def combine(slot_tok, slot_gate, counts, rows, extra, toks):
    cap, width = rows[0].shape[1:]
    lanes = width // 128

    def spec(which):
        return pl.BlockSpec((1, cap, width), lambda i, *_: (jnp.clip(i - 4 * which, 0, 3), 0, 0))

    whole = pl.BlockSpec((toks, width), lambda i, *_: (0, 0))
    return pl.pallas_call(
        combine_body,
        grid_spec=pltpu.PrefetchScalarGridSpec(
            num_scalar_prefetch=3,
            grid=(16,),
            in_specs=[spec(which) for which in range(4)] + [whole] * len(extra),
            out_specs=whole,
            scratch_shapes=[pltpu.VMEM(((toks + 1) * lanes, 128), F32), pltpu.VMEM((16 * lanes, 128), F32)],
        ),
        out_shape=jax.ShapeDtypeStruct((toks, width), F32),
        compiler_params=pltpu.CompilerParams(vmem_limit_bytes=48 * 2**20),
        cost_estimate=pl.CostEstimate(flops=10_000_000_000, bytes_accessed=20_000_000, transcendentals=0),
        name="combine",
    )(slot_tok, slot_gate, counts, *rows, *extra)


def shared_body(rows_ref, gate_ref, up_ref, down_ref, out_ref):
    rows = rows_ref[...]
    hidden = (jax.nn.silu(dot32(rows, gate_ref[...])) * dot32(rows, up_ref[...])).astype(BF16)
    part = dot32(hidden, down_ref[...])

    @pl.when(pl.program_id(0) == 0)
    def _():
        out_ref[...] = part

    @pl.when(pl.program_id(0) > 0)
    def _():
        out_ref[...] += part


def shared_experts(rows, ws_gate, ws_up, ws_down):
    toks, width = rows.shape
    inner = ws_gate.shape[1]
    blk = 256
    return pl.pallas_call(
        shared_body,
        grid=(inner // blk,),
        in_specs=[
            pl.BlockSpec((toks, width), lambda f: (0, 0)),
            pl.BlockSpec((width, blk), lambda f: (0, f)),
            pl.BlockSpec((width, blk), lambda f: (0, f)),
            pl.BlockSpec((blk, width), lambda f: (f, 0)),
        ],
        out_specs=pl.BlockSpec((toks, width), lambda f: (0, 0)),
        out_shape=jax.ShapeDtypeStruct((toks, width), F32),
        cost_estimate=pl.CostEstimate(flops=6 * toks * width * inner, bytes_accessed=50_000_000, transcendentals=0),
        name="shared",
    )(rows, ws_gate, ws_up, ws_down)


def route_slots(ids, gates, expert_count, cap):
    toks = ids.shape[0]
    hits = ids[:, :, None] == jnp.arange(expert_count)[None, None, :]
    member = jnp.any(hits, axis=1)
    gate_of = jnp.sum(jnp.where(hits, gates[:, :, None], 0.0), axis=1)
    earlier = (jnp.arange(toks)[:, None] > jnp.arange(toks)[None, :]).astype(BF16)
    rank = dot32(earlier, member.astype(BF16)).astype(jnp.int32)
    key = jnp.where(member, rank, -1)
    match = key[:, None, :] == jnp.arange(cap)[None, :, None]
    tok_num = (jnp.arange(toks, dtype=F32) - toks)[:, None, None]
    slot_tok = jnp.sum(jnp.where(match, tok_num, 0.0), axis=0) + toks
    slot_gate = jnp.sum(jnp.where(match, gate_of[:, None, :], 0.0), axis=0)
    return jnp.stack([slot_tok.T, slot_gate.T])


def solution(mesh):
    tp_size = mesh.shape['tp']
    ep_size = mesh.shape['ep']
    token_spec = P('ep', 'tp', None)
    expert_spec = P(('tp', 'ep'), None, None)
    in_specs = (token_spec, token_spec, token_spec, P(None), P(None, 'tp'), P(None, None), P(None), P(None, 'tp'), P('tp', None), P(None), expert_spec, expert_spec, expert_spec, P(None, None), P(None, None), P(None, None))
    core, flip_x, flip_y = 1, 2, 4

    def swap(values, mask):
        return lax.ppermute(values, 'ep', [(i, i ^ mask) for i in range(ep_size)])

    def from_plane(values, ahead):
        return lax.ppermute(values, 'tp', [((i + ahead) % tp_size, i) for i in range(tp_size)])

    def to_plane(values, ahead):
        return lax.ppermute(values, 'tp', [(i, (i + ahead) % tp_size) for i in range(tp_size)])

    def gather_weight(shard):
        piece_rows = shard.shape[0] // ep_size
        piece = lax.dynamic_slice_in_dim(shard, lax.axis_index('ep') * piece_rows, piece_rows, axis=0)
        full = lax.all_gather(piece, ('tp', 'ep'), axis=0, tiled=True)
        return full.reshape((tp_size,) + shard.shape)

    def layer(x_in, topk_idx, top_gate, g_attn, w_q, w_dkv, g_kv, w_ukv, w_o, g_ffn, w_gate, w_up, w_down, ws_gate, ws_up, ws_down):
        dims = model_dims(w_q, w_dkv, g_kv, w_ukv, w_o)
        kv_rank, rope_dim, heads, _, value_dim = dims
        expert_count = w_gate.shape[0]
        top_k = topk_idx.shape[-1]

        def device_work(x_loc, ids_loc, gate_loc, g_attn, w_q, w_dkv, g_kv, w_ukv, w_o, g_ffn, w_gate, w_up, w_down, ws_gate, ws_up, ws_down):
            bat, seq_loc, width = x_loc.shape
            toks = bat * seq_loc
            limit = 3 * (toks * top_k // expert_count)
            cap = -(-limit // 32) * 32
            z_idx = lax.axis_index('tp')
            ep_idx = lax.axis_index('ep')

            chunks = w_q.shape[0] // kv_rank
            q_cols = w_q.shape[1]
            packed = jnp.concatenate([w_ukv] + [w_q[part * kv_rank:(part + 1) * kv_rank] for part in range(chunks)], axis=1)
            packed = gather_weight(packed)
            full_o = gather_weight(w_o)
            weights = [w_gate, w_up, w_down] + [swap(w, core) for w in (w_gate, w_up, w_down)]

            x_rows = x_loc.reshape(toks, width)
            normed = rms_norm(x_rows, g_attn)
            latent = dot32(normed, w_dkv)
            cos_tab, sin_tab = rope_tables(z_idx * seq_loc + jnp.arange(seq_loc), rope_dim)
            c_kv = rms_norm(latent[:, :kv_rank], g_kv).reshape(bat, seq_loc, kv_rank)
            k_rope = rotate(latent[:, kv_rank:].reshape(bat, seq_loc, rope_dim), cos_tab, sin_tab)
            cache_loc = jnp.concatenate([c_kv, k_rope], axis=-1)
            caches = [cache_loc] + [from_plane(cache_loc, ahead) for ahead in range(1, tp_size)]

            masks = (0, flip_x, flip_y, flip_x | flip_y)
            slots = route_slots(ids_loc.reshape(toks, top_k), gate_loc.reshape(toks, top_k), expert_count, cap)
            slots = slots.reshape(2, tp_size, expert_count // tp_size, cap)
            plane_experts = jnp.concatenate([jnp.stack([2 * ((ep_idx ^ mask) ^ (j >> 1)) + (j & 1) for j in range(4)]) for mask in masks])
            homes = []
            for ahead in range(tp_size):
                mine = lax.dynamic_index_in_dim(slots, lax.rem(z_idx + tp_size - ahead, tp_size), axis=1, keepdims=False)
                homes.append((mine if ahead == 0 else from_plane(mine, ahead))[:, plane_experts])
            homes = jnp.stack(homes)
            toks_by_chip = homes[:, 0].astype(jnp.int32).reshape(tp_size, 4, 4, cap)
            wanted = jnp.stack([toks_by_chip[:, 0]] + [swap(toks_by_chip[:, which], masks[which]) for which in range(1, 4)], axis=2)
            small_all = (jnp.max(jnp.sum(wanted < toks, axis=3), axis=2) <= SMALL).astype(jnp.int32)
            home_cnt = jnp.sum(toks_by_chip < toks, axis=3).astype(jnp.int32).reshape(tp_size, 16)

            query = project(normed, packed, w_ukv.shape[1], q_cols)
            z_one = z_idx.astype(jnp.int32).reshape(1)
            heads_out = attend(query, caches, packed, z_one, cos_tab, sin_tab, dims)
            attn = dot32(heads_out, full_o.reshape(heads * value_dim, width)).astype(BF16)
            hidden = (x_rows.astype(F32) + attn.astype(F32)).astype(BF16)
            normed2 = rms_norm(hidden, g_ffn)

            half = toks // 2
            low, high = normed2[:half], normed2[half:]
            blocks = {}
            for ahead in (0, 2, 1, 3):
                lo = low if ahead == 0 else from_plane(low, ahead)
                hi = high if ahead == 0 else from_plane(high, ahead)
                lo_x, hi_y = swap(lo, flip_x), swap(hi, flip_y)
                lo_y, hi_x = swap(lo, flip_y), swap(hi, flip_x)
                lo_d, hi_d = swap(lo_x, flip_y), swap(hi_y, flip_x)
                blocks[ahead] = [lo, hi, lo_x, hi_x, lo_y, hi_y, lo_d, hi_d]

            shared_out = shared_experts(normed2, ws_gate, ws_up, ws_down)
            extra = {0: (), 1: (), 2: (), 3: ()}
            total = hidden.astype(F32) + shared_out
            for ahead in (2, 1, 3, 0):
                ids_wide = jnp.broadcast_to(wanted[ahead].reshape(16, cap)[:, :, None], (16, cap, 128))
                mine = experts(small_all[ahead], ids_wide, blocks[ahead], weights, cap)
                rows = [mine[0]] + [swap(mine[which], masks[which]) for which in range(1, 4)]
                part = combine(toks_by_chip[ahead].reshape(-1), homes[ahead, 1].reshape(-1), home_cnt[ahead], rows, extra[ahead], toks)
                if ahead == 2:
                    up = lax.ppermute(part, 'tp', [(i, i + 1) for i in range(tp_size // 2)])
                    down = lax.ppermute(part, 'tp', [(i, i - 1) for i in range(tp_size // 2, tp_size)])
                    extra[1], extra[3] = (up,), (down,)
                else:
                    total = total + (part if ahead == 0 else to_plane(part, ahead))
            y_loc = total.astype(BF16).reshape(bat, seq_loc, width)
            return y_loc, cache_loc

        return jax.shard_map(device_work, mesh=mesh, in_specs=in_specs, out_specs=(token_spec, token_spec), check_vma=False)(x_in, topk_idx, top_gate, g_attn, w_q, w_dkv, g_kv, w_ukv, w_o, g_ffn, w_gate, w_up, w_down, ws_gate, ws_up, ws_down)

    return layer
```

```python
import functools

import jax
import jax.numpy as jnp
from jax import lax
from jax.experimental import pallas as pl
from jax.experimental.pallas import tpu as pltpu
from jax.sharding import PartitionSpec as P


F32 = jnp.float32
BF16 = jnp.bfloat16
VMEM_MAX = 67043328
SMALL = 32


def rms_norm(values, gain_vec):
    values32 = values.astype(F32)
    inv_rms = lax.rsqrt(jnp.mean(values32 * values32, axis=-1, keepdims=True) + 1e-6)
    return (values32 * inv_rms * gain_vec.astype(F32)).astype(BF16)


def rope_tables(positions, rope_dim):
    half_dim = rope_dim // 2
    inv_freq = 10000.0 ** (-2.0 * jnp.arange(half_dim, dtype=F32) / rope_dim)
    angles = positions.astype(F32)[:, None] * inv_freq[None, :]
    return jnp.cos(angles), jnp.sin(angles)


def rotate(values, cos_tab, sin_tab):
    half_dim = values.shape[-1] // 2
    first = values[..., :half_dim].astype(F32)
    second = values[..., half_dim:].astype(F32)
    return jnp.concatenate([first * cos_tab - second * sin_tab, second * cos_tab + first * sin_tab], axis=-1).astype(BF16)


def model_dims(w_q, w_dkv, g_kv, w_ukv, w_o):
    kv_rank = g_kv.shape[0]
    rope_dim = w_dkv.shape[1] - kv_rank
    heads = (w_q.shape[1] - w_ukv.shape[1] + w_o.shape[0]) // rope_dim
    return kv_rank, rope_dim, heads, w_q.shape[1] // heads - rope_dim, w_o.shape[0] // heads


def dot32(lhs, rhs):
    return jnp.dot(lhs, rhs, preferred_element_type=F32)


def latent_body(rank, x_ref, gain_ref, w_ref, gain_kv_ref, cos_ref, sin_ref, u_ref, cache_ref):
    normed = rms_norm(x_ref[0], gain_ref[...])
    u_ref[...] = normed
    latent = dot32(normed, w_ref[...])
    cache_ref[0, :, :rank] = rms_norm(latent[:, :rank], gain_kv_ref[...])
    cache_ref[0, :, rank:] = rotate(latent[:, rank:], cos_ref[...], sin_ref[...])


def latents(x_loc, g_attn, w_dkv, g_kv, cos_tab, sin_tab):
    bat, seq, width = x_loc.shape
    rank, wide = g_kv.shape[0], w_dkv.shape[1]
    half_rope = (wide - rank) // 2
    return pl.pallas_call(
        functools.partial(latent_body, rank),
        grid=(bat,),
        in_specs=[
            pl.BlockSpec((1, seq, width), lambda b: (b, 0, 0)),
            pl.BlockSpec((1, width), lambda b: (0, 0)),
            pl.BlockSpec((width, wide), lambda b: (0, 0)),
            pl.BlockSpec((1, rank), lambda b: (0, 0)),
            pl.BlockSpec((seq, half_rope), lambda b: (0, 0)),
            pl.BlockSpec((seq, half_rope), lambda b: (0, 0)),
        ],
        out_specs=[pl.BlockSpec((seq, width), lambda b: (b, 0)), pl.BlockSpec((1, seq, wide), lambda b: (b, 0, 0))],
        out_shape=[jax.ShapeDtypeStruct((bat * seq, width), BF16), jax.ShapeDtypeStruct((bat, seq, wide), BF16)],
        cost_estimate=pl.CostEstimate(flops=2 * bat * seq * width * wide, bytes_accessed=12_000_000, transcendentals=0),
        name="latents",
    )(x_loc, g_attn.reshape(1, width), w_dkv, g_kv.reshape(1, rank), cos_tab, sin_tab)


def group_body(dims, own, last, where_ref, u_ref, c0, c1, c2, c3, cos_ref, sin_ref, *refs):
    rank, rope, _, nope, vdim = dims
    weights, refs = (refs[:3], refs[3:]) if own else (refs[:2], refs[2:])
    prev, refs = (None, refs) if own else (refs[0], refs[1:])
    extras, refs = (refs[:2], refs[2:]) if last else ((), refs)
    outs, (w_q, w_kv, w_o, sem) = refs[:-4], refs[-4:]
    rows, blk = u_ref.shape[0], c0.shape[1]
    scale = (nope + rope) ** -0.5
    z_idx, ep_idx = where_ref[0], where_ref[1]

    @pl.when(pl.program_id(0) == 0)
    def _():
        copies = []
        if own:
            for index, dst in enumerate((w_q, w_kv, w_o)):
                copies.append(pltpu.make_async_copy(weights[index], dst, sem.at[index]))
        else:
            q_rows, kv_rows = w_q.shape[0] // 8, w_kv.shape[0] // 8
            cols = w_q.shape[1]
            kv_cols, o_cols = w_kv.shape[1], w_o.shape[1]
            spans = []
            for part in range((kv_cols + o_cols) // cols):
                lo, hi = part * cols, (part + 1) * cols
                if lo < kv_cols:
                    spans.append((part, 0, w_kv, lo, min(hi, kv_cols)))
                if hi > kv_cols:
                    spans.append((part, max(lo, kv_cols) - lo, w_o, max(lo, kv_cols) - kv_cols, hi - kv_cols))
            for mask in range(8):
                src = weights[mask & 1].at[mask >> 1]
                block = ep_idx ^ mask
                q_at = pl.ds(pl.multiple_of(block * q_rows, q_rows), q_rows)
                kv_at = pl.ds(pl.multiple_of(block * kv_rows, kv_rows), kv_rows)
                copies.append(pltpu.make_async_copy(src.at[:q_rows], w_q.at[q_at], sem.at[len(copies)]))
                for part, first, dst, lo, hi in spans:
                    top = q_rows + part * kv_rows
                    copies.append(pltpu.make_async_copy(src.at[top:top + kv_rows, first:first + hi - lo], dst.at[kv_at, lo:hi], sem.at[len(copies)]))
        for copy in copies:
            copy.start()
        for copy in copies:
            copy.wait()

    query = dot32(u_ref[...], w_q[...]).astype(BF16)
    cache = jnp.concatenate([c0[0], c1[0], c2[0], c3[0]], axis=0)
    key_val = dot32(cache[:, :rank], w_kv[...]).astype(BF16)
    k_rope = cache[:, rank:]
    fold = scale * 1.4426950408889634
    ahead = lax.broadcasted_iota(jnp.int32, (1, 3 * blk), 1) // blk + 1
    hidden_keys = jnp.where(z_idx + ahead >= 4, 0.0, -jnp.inf)
    causal = lax.broadcasted_iota(jnp.int32, (rows, blk), 0) >= lax.broadcasted_iota(jnp.int32, (rows, blk), 1)
    cos_tab, sin_tab = cos_ref[...], sin_ref[...]
    contract = (((1,), (1,)), ((), ()))
    heads_out = []
    for head in range(w_q.shape[1] // (nope + rope)):
        base = head * (nope + rope)
        q_rope = rotate(query[:, base + nope:base + nope + rope], cos_tab, sin_tab)
        q_head = jnp.concatenate([query[:, base:base + nope], q_rope], axis=1)
        start = head * (nope + vdim)
        k_head = jnp.concatenate([key_val[:, start:start + nope], k_rope], axis=1)
        value = key_val[:, start + nope:start + nope + vdim]
        here = lax.dot_general(q_head, k_head[:blk], contract, preferred_element_type=F32)
        here = jnp.where(causal, here, -jnp.inf)
        there = lax.dot_general(q_head, k_head[blk:], contract, preferred_element_type=F32) + hidden_keys
        top = jnp.maximum(jnp.max(here, axis=-1, keepdims=True), jnp.max(there, axis=-1, keepdims=True))
        here, there = jnp.exp2((here - top) * fold), jnp.exp2((there - top) * fold)
        inv = 1.0 / (jnp.sum(here, axis=-1, keepdims=True) + jnp.sum(there, axis=-1, keepdims=True))
        head_out = dot32((here * inv).astype(BF16), value[:blk]) + dot32((there * inv).astype(BF16), value[blk:])
        heads_out.append(head_out.astype(BF16))
    total = dot32(jnp.concatenate(heads_out, axis=1), w_o[...])
    if prev is not None:
        total = total + prev[...]
    if last:
        hidden = (extras[0][0].astype(F32) + total.astype(BF16).astype(F32)).astype(BF16)
        outs[0][...] = hidden
        outs[1][...] = rms_norm(hidden, extras[1][...])
    else:
        outs[0][...] = total


def attend_group(where, u_rows, caches, cos_tab, sin_tab, weights, prev, extras, dims, shapes):
    _, rope, _, _, _ = dims
    bat, blk, wide = caches[0].shape
    width = u_rows.shape[1]
    own, last = prev is None, bool(extras)
    tok_spec = pl.BlockSpec((blk, width), lambda b: (b, 0))
    table = pl.BlockSpec((blk, rope // 2), lambda b: (0, 0))
    in_specs = [pl.BlockSpec(memory_space=pltpu.SMEM), tok_spec] + [pl.BlockSpec((1, blk, wide), lambda b: (b, 0, 0))] * 4 + [table, table]
    in_specs += [pl.BlockSpec(memory_space=pl.ANY)] * len(weights)
    args = [where, u_rows, *caches, cos_tab, sin_tab, *weights]
    if not own:
        in_specs.append(tok_spec)
        args.append(prev)
    if last:
        in_specs += [pl.BlockSpec((1, blk, width), lambda b: (b, 0, 0)), pl.BlockSpec((1, width), lambda b: (0, 0))]
        args += list(extras)
    out = jax.ShapeDtypeStruct(u_rows.shape, BF16 if last else F32)
    return pl.pallas_call(
        functools.partial(group_body, dims, own, last),
        grid=(bat,),
        in_specs=in_specs,
        out_specs=[tok_spec] * (2 if last else 1),
        out_shape=[out] * (2 if last else 1),
        scratch_shapes=[pltpu.VMEM(shape, BF16) for shape in shapes] + [pltpu.SemaphoreType.DMA((48,))],
        compiler_params=pltpu.CompilerParams(vmem_limit_bytes=VMEM_MAX),
        cost_estimate=pl.CostEstimate(flops=15_000_000_000, bytes_accessed=30_000_000, transcendentals=0),
        name="attend",
    )(*args)


def experts_body(half, small_ref, ids_ref, *refs):
    toks, (gate_a, up_a, down_a, gate_b, up_b, down_b) = refs[:8], refs[8:14]
    outs = refs[14:18]
    tok, gate_up, down, stage, few, tok_sem, in_sem, down_sem, out_sem = refs[18:]
    step = pl.program_id(0)
    width = gate_a.shape[2]
    cap = stage.shape[1]
    tok_count = tok.shape[1]

    def load_gate_up(which):
        slot = which % 2
        src = (gate_a, up_a) if which < 2 else (gate_b, up_b)
        for part in range(2):
            pltpu.make_async_copy(src[part].at[which % 2], gate_up.at[slot, :, part * width:(part + 1) * width], in_sem.at[slot, part]).start()

    def load_down(which):
        src = down_a if which < 2 else down_b
        pltpu.make_async_copy(src.at[which % 2], down.at[which % 2], down_sem.at[which % 2]).start()

    @pl.when(step == 0)
    def _():
        load_gate_up(0)
        for index in range(8):
            pltpu.make_async_copy(toks[index], tok.at[index // 2, (index % 2) * half:(index % 2 + 1) * half], tok_sem.at[index]).start()
        load_down(0)

    for which in range(1, 4):
        @pl.when(step == which - 1)
        def _():
            load_gate_up(which)
            load_down(which)

    @pl.when(step == 0)
    def _():
        for index in range(8):
            pltpu.make_async_copy(toks[index], tok.at[index // 2, (index % 2) * half:(index % 2 + 1) * half], tok_sem.at[index]).wait()

    for which in range(4):
        @pl.when(step == which)
        def _():
            slot = which % 2
            for part in range(2):
                pltpu.make_async_copy(gate_a.at[0], gate_up.at[slot, :, part * width:(part + 1) * width], in_sem.at[slot, part]).wait()
            pltpu.make_async_copy(down_a.at[0], down.at[slot], down_sem.at[slot]).wait()

    now = lax.rem(step, 2)

    def mlp(rows):
        both = dot32(rows, gate_up[now])
        hidden = (jax.nn.silu(both[:, :width]) * both[:, width:]).astype(BF16)
        return dot32(hidden, down[now]).astype(BF16)

    def pick(home, count):
        ids = ids_ref[home, :count, :]
        lane = lax.broadcasted_iota(jnp.int32, ids.shape, 1)
        parts = [jnp.where(ids == lane + 128 * blk, 1.0, 0.0).astype(BF16) for blk in range(tok_count // 128)]
        return dot32(jnp.concatenate(parts, axis=1), tok[home]).astype(BF16)

    is_small = small_ref[step] == 1

    @pl.when(is_small)
    def _():
        few[...] = mlp(jnp.concatenate([pick(home, SMALL) for home in range(4)], axis=0))

    @pl.loop(0, 4)
    def _(home):
        slot = lax.rem(home, 2)

        @pl.when(jnp.logical_or(step > 0, home >= 2))
        def _():
            pltpu.make_async_copy(stage.at[slot], outs[0].at[0], out_sem.at[slot]).wait()

        @pl.when(is_small)
        def _():
            stage[slot, :SMALL, :] = few[pl.ds(pl.multiple_of(home * SMALL, SMALL), SMALL), :]

        @pl.when(jnp.logical_not(is_small))
        def _():
            stage[slot] = mlp(pick(home, cap))

        for which in range(4):
            @pl.when(home == which)
            def _():
                pltpu.make_async_copy(stage.at[slot], outs[which].at[step], out_sem.at[slot]).start()

    @pl.when(step == 3)
    def _():
        for slot in range(2):
            pltpu.make_async_copy(stage.at[slot], outs[0].at[0], out_sem.at[slot]).wait()


def experts(small, ids, toks, weights, cap):
    half, width = toks[0].shape
    ff = weights[0].shape[2]
    hbm = pl.BlockSpec(memory_space=pl.ANY)
    return pl.pallas_call(
        functools.partial(experts_body, half),
        grid=(4,),
        in_specs=[pl.BlockSpec(memory_space=pltpu.SMEM), pl.BlockSpec((4, cap, 128), lambda e: (e, 0, 0))] + [hbm] * 14,
        out_specs=[hbm] * 4,
        out_shape=[jax.ShapeDtypeStruct((4, cap, width), BF16)] * 4,
        scratch_shapes=[
            pltpu.VMEM((4, 2 * half, width), BF16),
            pltpu.VMEM((2, width, 2 * ff), BF16),
            pltpu.VMEM((2, ff, width), BF16),
            pltpu.VMEM((2, cap, width), BF16),
            pltpu.VMEM((4 * SMALL, width), BF16),
            pltpu.SemaphoreType.DMA((8,)),
            pltpu.SemaphoreType.DMA((2, 2)),
            pltpu.SemaphoreType.DMA((2,)),
            pltpu.SemaphoreType.DMA((2,)),
        ],
        compiler_params=pltpu.CompilerParams(vmem_limit_bytes=VMEM_MAX),
        cost_estimate=pl.CostEstimate(flops=60_000_000_000, bytes_accessed=100_000_000, transcendentals=0),
        name="experts",
    )(small, ids, *toks, *weights)


def combine_body(tok_ref, gate_ref, cnt_ref, r0, r1, r2, r3, *rest):
    extra, (out_ref, acc, turn) = rest[:-3], rest[-3:]
    step = pl.program_id(0)
    cap, width = r0.shape[1], r0.shape[2]
    lanes = width // 128
    toks = out_ref.shape[0]

    @pl.when(step == 0)
    def _():
        acc[...] = jnp.zeros_like(acc)

    for which, src in enumerate((r0, r1, r2, r3)):
        @pl.when(step // 4 == which)
        def _():
            @pl.loop(0, (cnt_ref[step] + 23) // 24)
            def _(group):
                first = pl.multiple_of(group * 24, 8)
                rows = src[0, pl.ds(first, 24), :].astype(F32)
                for blk in range(lanes):
                    turn[pl.ds(blk, 24, stride=lanes), :] = rows[:, 128 * blk:128 * (blk + 1)]
                base = step * cap + first
                for part in range(0, 24, 8):
                    spots = [pl.multiple_of(tok_ref[base + part + r] * lanes, lanes) for r in range(8)]
                    olds = [acc[pl.ds(spot, lanes), :] for spot in spots]
                    news = [olds[r] + gate_ref[base + part + r] * turn[(part + r) * lanes:(part + r + 1) * lanes, :] for r in range(8)]
                    for r in range(8):
                        acc[pl.ds(spots[r], lanes), :] = news[r]

    @pl.when(step == 15)
    def _():
        @pl.loop(0, toks // 8)
        def _(tile):
            first = pl.multiple_of(tile * 8, 8)
            for blk in range(lanes):
                value = acc[pl.ds(first * lanes + blk, 8, stride=lanes), :]
                for more in extra:
                    value = value + more[pl.ds(first, 8), 128 * blk:128 * (blk + 1)]
                out_ref[pl.ds(first, 8), 128 * blk:128 * (blk + 1)] = value


def combine(slot_tok, slot_gate, counts, rows, extra, toks):
    cap, width = rows[0].shape[1:]
    lanes = width // 128

    def spec(which):
        return pl.BlockSpec((1, cap, width), lambda i, *_: (jnp.clip(i - 4 * which, 0, 3), 0, 0))

    whole = pl.BlockSpec((toks, width), lambda i, *_: (0, 0))
    return pl.pallas_call(
        combine_body,
        grid_spec=pltpu.PrefetchScalarGridSpec(
            num_scalar_prefetch=3,
            grid=(16,),
            in_specs=[spec(which) for which in range(4)] + [whole] * len(extra),
            out_specs=whole,
            scratch_shapes=[pltpu.VMEM(((toks + 1) * lanes, 128), F32), pltpu.VMEM((24 * lanes, 128), F32)],
        ),
        out_shape=jax.ShapeDtypeStruct((toks, width), F32),
        compiler_params=pltpu.CompilerParams(vmem_limit_bytes=48 * 2**20),
        cost_estimate=pl.CostEstimate(flops=10_000_000_000, bytes_accessed=20_000_000, transcendentals=0),
        name="combine",
    )(slot_tok, slot_gate, counts, *rows, *extra)


def shared_body(rows_ref, gate_ref, up_ref, down_ref, out_ref):
    rows = rows_ref[...]
    hidden = (jax.nn.silu(dot32(rows, gate_ref[...])) * dot32(rows, up_ref[...])).astype(BF16)
    part = dot32(hidden, down_ref[...])

    @pl.when(pl.program_id(0) == 0)
    def _():
        out_ref[...] = part

    @pl.when(pl.program_id(0) > 0)
    def _():
        out_ref[...] += part


def shared_experts(rows, ws_gate, ws_up, ws_down):
    toks, width = rows.shape
    inner = ws_gate.shape[1]
    blk = 256
    return pl.pallas_call(
        shared_body,
        grid=(inner // blk,),
        in_specs=[
            pl.BlockSpec((toks, width), lambda f: (0, 0)),
            pl.BlockSpec((width, blk), lambda f: (0, f)),
            pl.BlockSpec((width, blk), lambda f: (0, f)),
            pl.BlockSpec((blk, width), lambda f: (f, 0)),
        ],
        out_specs=pl.BlockSpec((toks, width), lambda f: (0, 0)),
        out_shape=jax.ShapeDtypeStruct((toks, width), F32),
        cost_estimate=pl.CostEstimate(flops=6 * toks * width * inner, bytes_accessed=50_000_000, transcendentals=0),
        name="shared",
    )(rows, ws_gate, ws_up, ws_down)


def route_slots(ids, gates, expert_count, cap):
    toks = ids.shape[0]
    hits = ids[:, :, None] == jnp.arange(expert_count)[None, None, :]
    member = jnp.any(hits, axis=1)
    gate_of = jnp.sum(jnp.where(hits, gates[:, :, None], 0.0), axis=1)
    earlier = (jnp.arange(toks)[:, None] > jnp.arange(toks)[None, :]).astype(BF16)
    rank = dot32(earlier, member.astype(BF16)).astype(jnp.int32)
    key = jnp.where(member, rank, -1)
    match = key[:, None, :] == jnp.arange(cap)[None, :, None]
    tok_num = (jnp.arange(toks, dtype=F32) - toks)[:, None, None]
    slot_tok = jnp.sum(jnp.where(match, tok_num, 0.0), axis=0) + toks
    slot_gate = jnp.sum(jnp.where(match, gate_of[:, None, :], 0.0), axis=0)
    return jnp.stack([slot_tok.T, slot_gate.T])


def solution(mesh):
    tp_size = mesh.shape['tp']
    ep_size = mesh.shape['ep']
    token_spec = P('ep', 'tp', None)
    expert_spec = P(('tp', 'ep'), None, None)
    in_specs = (token_spec, token_spec, token_spec, P(None), P(None, 'tp'), P(None, None), P(None), P(None, 'tp'), P('tp', None), P(None), expert_spec, expert_spec, expert_spec, P(None, None), P(None, None), P(None, None))
    core, flip_x, flip_y = 1, 2, 4

    def swap(values, mask):
        return lax.ppermute(values, 'ep', [(i, i ^ mask) for i in range(ep_size)])

    def from_plane(values, ahead):
        return lax.ppermute(values, 'tp', [((i + ahead) % tp_size, i) for i in range(tp_size)])

    def to_plane(values, ahead):
        return lax.ppermute(values, 'tp', [(i, (i + ahead) % tp_size) for i in range(tp_size)])

    def relay(one, three):
        half_tp = tp_size // 2
        down = lax.ppermute(one, 'tp', [(i + 1, i) for i in range(half_tp)])
        up = lax.ppermute(three, 'tp', [(i - 1, i) for i in range(half_tp, tp_size)])
        return jnp.where(lax.axis_index('tp') < half_tp, down, up)

    def layer(x_in, topk_idx, top_gate, g_attn, w_q, w_dkv, g_kv, w_ukv, w_o, g_ffn, w_gate, w_up, w_down, ws_gate, ws_up, ws_down):
        dims = model_dims(w_q, w_dkv, g_kv, w_ukv, w_o)
        kv_rank, rope_dim, _, _, _ = dims
        expert_count = w_gate.shape[0]
        top_k = topk_idx.shape[-1]

        def device_work(x_loc, ids_loc, gate_loc, g_attn, w_q, w_dkv, g_kv, w_ukv, w_o, g_ffn, w_gate, w_up, w_down, ws_gate, ws_up, ws_down):
            bat, seq_loc, width = x_loc.shape
            toks = bat * seq_loc
            limit = 3 * (toks * top_k // expert_count)
            cap = -(-limit // 24) * 24
            z_idx = lax.axis_index('tp')
            ep_idx = lax.axis_index('ep')

            q_rows, kv_rows = width // ep_size, kv_rank // ep_size
            q_cols = w_q.shape[1]
            rest = jnp.concatenate([lax.dynamic_slice_in_dim(w, ep_idx * kv_rows, kv_rows, axis=0) for w in (w_ukv, w_o)], axis=1)
            parts = [lax.dynamic_slice_in_dim(w_q, ep_idx * q_rows, q_rows, axis=0)]
            parts += [rest[:, first:first + q_cols] for first in range(0, rest.shape[1], q_cols)]
            piece = jnp.concatenate(parts, axis=0)
            quads, pairs, at_zs = {}, {}, {}
            for ahead in (1, 3, 2):
                at_z = relay(at_zs[1], at_zs[3]) if ahead == 2 else from_plane(piece, ahead)
                at_zs[ahead] = at_z
                at_x, at_y = swap(at_z, flip_x), swap(at_z, flip_y)
                if ahead == 2:
                    at_d = swap(at_z, flip_x | flip_y)
                else:
                    at_d = swap(at_y, flip_x) if ahead == 3 else swap(at_x, flip_y)
                quads[ahead] = jnp.stack([at_z, at_x, at_y, at_d])
                pairs[ahead] = swap(quads[ahead], core)
            weights = [w_gate, w_up, w_down] + [swap(w, core) for w in (w_gate, w_up, w_down)]

            cos_tab, sin_tab = rope_tables(z_idx * seq_loc + jnp.arange(seq_loc), rope_dim)
            u_rows, cache_loc = latents(x_loc, g_attn, w_dkv, g_kv, cos_tab, sin_tab)
            cache_1, cache_3 = from_plane(cache_loc, 1), from_plane(cache_loc, 3)
            caches = [cache_loc, cache_1, relay(cache_1, cache_3), cache_3]

            masks = (0, flip_x, flip_y, flip_x | flip_y)
            slots = route_slots(ids_loc.reshape(toks, top_k), gate_loc.reshape(toks, top_k), expert_count, cap)
            slots = slots.reshape(2, tp_size, expert_count // tp_size, cap)
            plane_experts = jnp.concatenate([jnp.stack([2 * ((ep_idx ^ mask) ^ (j >> 1)) + (j & 1) for j in range(4)]) for mask in masks])
            homes = []
            for ahead in range(tp_size):
                mine = lax.dynamic_index_in_dim(slots, lax.rem(z_idx + tp_size - ahead, tp_size), axis=1, keepdims=False)
                homes.append((mine if ahead == 0 else from_plane(mine, ahead))[:, plane_experts])
            homes = jnp.stack(homes)
            toks_by_chip = homes[:, 0].astype(jnp.int32).reshape(tp_size, 4, 4, cap)
            wanted = jnp.stack([toks_by_chip[:, 0]] + [swap(toks_by_chip[:, which], masks[which]) for which in range(1, 4)], axis=2)
            small_all = (jnp.max(jnp.sum(wanted < toks, axis=3), axis=2) <= SMALL).astype(jnp.int32)
            home_cnt = jnp.sum(toks_by_chip < toks, axis=3).astype(jnp.int32).reshape(tp_size, 16)

            where = jnp.stack([z_idx, ep_idx]).astype(jnp.int32)
            shapes = (w_q.shape, w_ukv.shape, w_o.shape)
            part = attend_group(where, u_rows, caches, cos_tab, sin_tab, (w_q, w_ukv, w_o), None, (), dims, shapes)[0]
            for ahead in (1, 3):
                part = attend_group(where, u_rows, caches, cos_tab, sin_tab, (quads[ahead], pairs[ahead]), part, (), dims, shapes)[0]
            extras = (x_loc, g_ffn.reshape(1, width))
            hidden, normed2 = attend_group(where, u_rows, caches, cos_tab, sin_tab, (quads[2], pairs[2]), part, extras, dims, shapes)

            half = toks // 2
            low, high = normed2[:half], normed2[half:]
            blocks = {}
            for ahead in (0, 2, 1):
                lo = low if ahead == 0 else from_plane(low, ahead)
                hi = high if ahead == 0 else from_plane(high, ahead)
                lo_x, hi_y = swap(lo, flip_x), swap(hi, flip_y)
                lo_y, hi_x = swap(lo, flip_y), swap(hi, flip_x)
                lo_d, hi_d = swap(lo_x, flip_y), swap(hi_y, flip_x)
                blocks[ahead] = [lo, hi, lo_x, hi_x, lo_y, hi_y, lo_d, hi_d]
            blocks[3] = [from_plane(block, 3) for block in blocks[0]]

            shared_out = shared_experts(normed2, ws_gate, ws_up, ws_down)
            extra = {0: (), 1: (), 2: (), 3: ()}
            base, late = hidden.astype(F32) + shared_out, None
            for ahead in (2, 1, 3, 0):
                ids_wide = jnp.broadcast_to(wanted[ahead].reshape(16, cap)[:, :, None], (16, cap, 128))
                mine = experts(small_all[ahead], ids_wide, blocks[ahead], weights, cap)
                rows = [mine[0]] + [swap(mine[which], masks[which]) for which in range(1, 4)]
                if ahead == 0:
                    extra[0] = (base,)
                part = combine(toks_by_chip[ahead].reshape(-1), homes[ahead, 1].reshape(-1), home_cnt[ahead], rows, extra[ahead], toks)
                if ahead == 2:
                    up = lax.ppermute(part, 'tp', [(i, i + 1) for i in range(tp_size // 2)])
                    down = lax.ppermute(part, 'tp', [(i, i - 1) for i in range(tp_size // 2, tp_size)])
                    extra[1], extra[3] = (up,), (down,)
                elif ahead == 1:
                    base = base + to_plane(part, 1)
                elif ahead == 3:
                    late = to_plane(part, 3)
            total = part + late
            y_loc = total.astype(BF16).reshape(bat, seq_loc, width)
            return y_loc, cache_loc

        return jax.shard_map(device_work, mesh=mesh, in_specs=in_specs, out_specs=(token_spec, token_spec), check_vma=False)(x_in, topk_idx, top_gate, g_attn, w_q, w_dkv, g_kv, w_ukv, w_o, g_ffn, w_gate, w_up, w_down, ws_gate, ws_up, ws_down)

    return layer
```
